32 devices in a mesh: replica: 4 (over z), tp: 8 (over y, x, core).
Axes of the slice: x: 2, y: 2, z: 4, core: 2. Of those that a mesh axis runs over, the one named last changes fastest.
Arguments:
- hidden: bfloat16 [256, 8192], P(('replica', 'tp')), may hold values from -64 to 64
- head: bfloat16 [152064, 8192], P(('replica', 'tp'))
- token_ids: int32 [256], replicated, may hold values from 0 to 152063
Outputs:
- logprob: float32 [256], P(('replica', 'tp'))
The draws below stay inside these ranges and needn't reach their ends.
All inputs are finite; a program needn't handle non-finite values.
Results may differ from the reference program's by a relative error of at most 0.0003.
Values may be sent and summed in bfloat16 or wider, within the bound.
A program may use at most 128 MiB of HBM per device.

```python
import math
import jax
import jax.numpy as jnp
from jax import lax

D = 8192
V = 152064
SEQS = 256


def head_row(key, index):
    values = jax.random.normal(jax.random.fold_in(key, index), (D,), jnp.float32)
    return jnp.clip(values, -6.0, 6.0) * (3.0 / math.sqrt(D))


def head_rows(key, indices):
    base = jax.random.fold_in(key, 11)
    return jax.vmap(lambda index: head_row(base, index))(indices)


def draw_head(key, part):
    return head_rows(key, jnp.arange(V, dtype=jnp.int32)).astype(jnp.bfloat16)


def draw_hidden(key, part):
    drawn = jnp.clip(jax.random.normal(jax.random.fold_in(key, 21), (SEQS, D), jnp.float32), -6.0, 6.0)
    return drawn.astype(jnp.bfloat16)


def place_ends(result, rng, smallest, largest):
    index_at = [jax.random.randint(jax.random.fold_in(rng, axis), (), 0, length) for axis, length in enumerate(result.shape)]
    main_axis = result.shape.index(max(result.shape))
    beside = index_at[:main_axis] + [(index_at[main_axis] + 1) % result.shape[main_axis]] + index_at[main_axis + 1:]
    return result.at[tuple(index_at)].set(smallest).at[tuple(beside)].set(largest)


def setup_inputs(seed: int = 0) -> dict:
    key_list = jax.random.split(jax.random.key(seed), 4)
    return {
        "hidden": draw_hidden(jax.random.fold_in(key_list[3], 71), 0),
        "head": draw_head(jax.random.fold_in(key_list[3], 71), 0),
        "token_ids": place_ends(jax.random.randint(key_list[2], (SEQS,), 0, V), jax.random.fold_in(key_list[2], 1), 0, V - 1).astype(jnp.int32),
    }


def reference(hidden, head, token_ids):
    logits = lax.dot_general(hidden, head, (((1,), (1,)), ((), ())), preferred_element_type=jnp.float32)
    row_top = jnp.max(logits, axis=1)
    row_total = jnp.sum(jnp.exp(logits - row_top[:, None]), axis=1)
    row_picked = jnp.take_along_axis(logits, token_ids[:, None].astype(jnp.int32), axis=1)[:, 0]
    return row_picked - row_top - jnp.log(row_total)
```

```python
import functools

import jax
import jax.numpy as jnp
from jax import lax
from jax.experimental import pallas as pl
from jax.experimental.pallas import tpu as pltpu
from jax.sharding import PartitionSpec as P

MESH = pl.DeviceIdType.MESH
SLICES = 4
PIECES = 2 * SLICES
VMEM = 66_000_000


def chunk_rows(rows, limit):
    return max((r for r in range(8, limit + 1, 8) if rows % r == 0), default=rows)


def split_axis(size):
    return (size // 4, 2, 2) if size % 4 == 0 else (size, 1, 1)


def kernel(dims, rows, slots, tokens_ref, hidden_ref, head_ref, out_ref, ring, acc, gathered, hid,
           stats, sent, arrived, ring_sem, own_sem, gsend, grecv, ssend, srecv):
    z_n, y_n, x_n, c_n = dims
    tp_n = y_n * x_n * c_n
    devices = z_n * tp_n
    z = lax.axis_index("replica")
    t = lax.axis_index("tp")
    me = z * tp_n + t
    y, x, c = t // (x_n * c_n), (t // c_n) % x_n, t % c_n
    at = (z, y, x, c)
    per_device, depth = hidden_ref.shape
    local_vocab = head_ref.shape[0]
    seqs = hid.shape[0]
    piece_k, slice_k = depth // PIECES, depth // SLICES
    chunks = local_vocab // rows
    blocks = chunks * SLICES

    def fetch(i, slot):
        s, k = i // chunks, i % chunks
        return pltpu.make_async_copy(
            head_ref.at[pl.ds(pl.multiple_of(k * rows, 8), rows), pl.ds(pl.multiple_of(s * slice_k, 128), slice_k)],
            ring.at[slot], ring_sem.at[slot])

    def own(p):
        return pltpu.make_async_copy(
            hidden_ref.at[:, pl.ds(p * piece_k, piece_k)], gathered.at[p, z, y, x, c], own_sem.at[p])

    for p in range(PIECES):
        own(p).start()

    @pl.loop(0, slots)
    def _(i):
        fetch(i, i).start()

    barrier = pltpu.get_barrier_semaphore()

    @pl.loop(1, devices)
    def _(k):
        d = (me + k) % devices
        pl.semaphore_signal(barrier, inc=1, device_id=(d // tp_n, d % tp_n), device_id_type=MESH)

    pl.semaphore_wait(barrier, devices - 1)

    def order(p):
        return (0, 1, 2, 3) if p % 2 == 0 else (0, 2, 1, 3)

    def copy(p, phase, k, incoming=False):
        path = order(p)
        axis = path[phase]
        n = dims[axis]
        there = list(at)
        there[axis] = (at[axis] + k) % n
        mine = at[axis] if not incoming else (at[axis] + n - k) % n
        index = [p]
        for a in range(4):
            if a in path[:phase]:
                index.append(slice(None))
            elif a == axis:
                index.append(mine)
            else:
                index.append(at[a])
        ref = gathered.at[tuple(index)]
        device = (there[0], (there[1] * x_n + there[2]) * c_n + there[3])
        return pltpu.make_async_remote_copy(
            src_ref=ref, dst_ref=ref, send_sem=gsend.at[p, phase, k - 1], recv_sem=grecv.at[p, phase, k - 1],
            device_id=device, device_id_type=MESH)

    def hops(p, phase):
        return range(1, dims[order(p)[phase]])

    def arrive(p, phase):
        for k in hops(p, phase):
            copy(p, phase, k, incoming=True).wait_recv()

    def step(s, phase):
        for p in (2 * s, 2 * s + 1):
            if phase == 0:
                own(p).wait()
            else:
                arrive(p, phase - 1)
            for k in hops(p, phase):
                copy(p, phase, k).start()

    def finish(s):
        for p in (2 * s, 2 * s + 1):
            arrive(p, 3)
            block = gathered[p].astype(jnp.float32).reshape(seqs, piece_k)
            hid[:, p * piece_k:(p + 1) * piece_k] = block.astype(jnp.bfloat16)

    stats[0:1, :] = jnp.full((1, seqs), -jnp.inf, jnp.float32)
    stats[1:3, :] = jnp.zeros((2, seqs), jnp.float32)

    def compute(s, low, high):
        def body(k, carry):
            i = s * chunks + k
            slot = i % slots
            fetch(i, slot).wait()
            part = lax.dot_general(ring[slot], hid[:, s * slice_k:(s + 1) * slice_k], (((1,), (1,)), ((), ())),
                                   preferred_element_type=jnp.float32)
            place = pl.ds(pl.multiple_of(k * rows, 8), rows)
            if s == 0:
                acc[place, :] = part
            elif s < SLICES - 1:
                acc[place, :] += part
            else:
                logits = acc[place, :] + part
                top = stats[0:1, :]
                new_top = jnp.maximum(top, jnp.max(logits, axis=0, keepdims=True))
                column = lax.broadcasted_iota(jnp.int32, logits.shape, 0) + (me * local_vocab + k * rows)
                hit = jnp.where(column == tokens_ref[...], logits, 0.0)
                total = jnp.sum(jnp.exp(logits - new_top), axis=0, keepdims=True)
                stats[0:1, :] = new_top
                stats[1:2, :] = stats[1:2, :] * jnp.exp(top - new_top) + total
                stats[2:3, :] += jnp.sum(hit, axis=0, keepdims=True)

            @pl.when(i + slots < blocks)
            def _():
                fetch(i + slots, slot).start()
            return carry
        lax.fori_loop(low, high, body, 0)

    for s in range(SLICES):
        step(s, 0)
    todo = [(s, w - s + 1) for w in range(3 + SLICES) for s in range(SLICES) if 1 <= w - s + 1 <= 3]
    first = todo.index((0, 3)) + 1
    for s, phase in todo[:first]:
        step(s, phase)
    rest = todo[first:]
    parts = max(1, min(chunks, len(rest)))
    edges = [chunks * j // parts for j in range(parts + 1)]
    finish(0)
    for j in range(parts):
        for s, phase in rest[len(rest) * j // parts:len(rest) * (j + 1) // parts]:
            step(s, phase)
        compute(0, edges[j], edges[j + 1])
    for s in range(1, SLICES):
        finish(s)
        compute(s, 0, chunks)

    line = lax.broadcasted_iota(jnp.int32, (128, seqs), 0)
    table = jnp.where(line == 0, stats[0:1, :], jnp.where(line == 1, stats[1:2, :], stats[2:3, :]))
    sent[...] = table.T.reshape(devices, per_device, 128)
    arrived[pl.ds(me, 1)] = sent[pl.ds(me, 1)]

    def result(k, incoming=False):
        d = (me + k) % devices
        origin = (me + devices - k) % devices if incoming else me
        return pltpu.make_async_remote_copy(
            src_ref=sent.at[d], dst_ref=arrived.at[origin], send_sem=ssend.at[k], recv_sem=srecv.at[k],
            device_id=(d // tp_n, d % tp_n), device_id_type=MESH)

    @pl.loop(1, devices)
    def _(k):
        result(k).start()

    for p in range(PIECES):
        for phase in range(4):
            for k in hops(p, phase):
                copy(p, phase, k).wait_send()

    @pl.loop(1, devices)
    def _(k):
        result(k, incoming=True).wait_recv()
        result(k).wait_send()

    table = arrived[...]
    tops, totals, picked = table[:, :, 0:1], table[:, :, 1:2], table[:, :, 2:3]
    top = jnp.max(tops, axis=0)
    total = jnp.sum(totals * jnp.exp(tops - top[None]), axis=0)
    value = jnp.sum(picked, axis=0) - top - jnp.log(total)
    out_ref[...] = jnp.broadcast_to(value, out_ref.shape)


def shards(z_n, tp_n, hidden, head, token_ids):
    dims = (z_n,) + split_axis(tp_n)
    devices = z_n * tp_n
    per_device, depth = hidden.shape
    seqs = per_device * devices
    rows = chunk_rows(head.shape[0], 528)
    blocks = head.shape[0] // rows * SLICES
    block_bytes = rows * depth // SLICES * 2
    fixed = head.shape[0] * seqs * 4 + 2 * seqs * depth * 2 + 2 * rows * seqs * 4 + 3 * 2**20
    slots = max(2, min(blocks, (VMEM - fixed) // block_bytes))
    hop_n = max(max(dims) - 1, 1)
    out = pl.pallas_call(
        functools.partial(kernel, dims, rows, slots),
        out_shape=jax.ShapeDtypeStruct((per_device, 128), jnp.float32),
        in_specs=[pl.BlockSpec(memory_space=pltpu.VMEM), pl.BlockSpec(memory_space=pltpu.HBM),
                  pl.BlockSpec(memory_space=pltpu.HBM)],
        out_specs=pl.BlockSpec(memory_space=pltpu.VMEM),
        scratch_shapes=[
            pltpu.VMEM((slots, rows, depth // SLICES), jnp.bfloat16),
            pltpu.VMEM((head.shape[0], seqs), jnp.float32),
            pltpu.VMEM((PIECES,) + dims + (per_device, depth // PIECES), jnp.bfloat16),
            pltpu.VMEM((seqs, depth), jnp.bfloat16),
            pltpu.VMEM((8, seqs), jnp.float32),
            pltpu.VMEM((devices, per_device, 128), jnp.float32),
            pltpu.VMEM((devices, per_device, 128), jnp.float32),
            pltpu.SemaphoreType.DMA((slots,)),
            pltpu.SemaphoreType.DMA((PIECES,)),
            pltpu.SemaphoreType.DMA((PIECES, 4, hop_n)),
            pltpu.SemaphoreType.DMA((PIECES, 4, hop_n)),
            pltpu.SemaphoreType.DMA((devices,)),
            pltpu.SemaphoreType.DMA((devices,)),
        ],
        compiler_params=pltpu.CompilerParams(
            collective_id=0, has_side_effects=True, vmem_limit_bytes=67_000_000),
    )(token_ids.reshape(1, seqs), hidden, head)
    return out[:, 0]


def solution(mesh):
    in_specs = (P(("replica", "tp"), None), P(("replica", "tp"), None), P())
    body = functools.partial(shards, mesh.shape["replica"], mesh.shape["tp"])
    return jax.shard_map(body, mesh=mesh, in_specs=in_specs, out_specs=P(("replica", "tp")), check_vma=False)
```
